128 devices in a mesh: dp: 32 (over z, y, x_lo), tensor: 4 (over x_hi, core).
Axes of the slice: x: 4 (x_hi: 2, x_lo: 2; x = x_hi * 2 + x_lo), y: 4, z: 4, core: 2. Of those that a mesh axis runs over, the one named last changes fastest.
Arguments:
- patches: bfloat16 [32768, 1280], P('dp'), may hold values from -27 to 27
- norm_gain: float32 [1280], replicated, may hold values from 0.1 to 1.9
- norm_bias: float32 [1280], replicated, may hold values from -3 to 3
- first_weight: bfloat16 [5120, 5120], P(None, 'tensor'), may hold values from -0.078125 to 0.078125
- first_bias: float32 [5120], P('tensor'), may hold values from -3 to 3
- second_weight: bfloat16 [5120, 8192], P('tensor', 'dp'), may hold values from -0.078125 to 0.078125
- second_bias: float32 [8192], P('tensor'), may hold values from -2 to 2
- text_embeds: bfloat16 [16384, 8192], P('dp', 'tensor'), may hold values from -36 to 36
- final_gain: float32 [8192], P('tensor'), may hold values from 0.1 to 1.9
- image_grids: int32 [32, 4, 2], replicated, may hold values from 2 to 8, as said below
- routing: int32 [32, 4], replicated, may hold values from 0 to 3, each once within a row
Outputs:
- embeddings: bfloat16 [16384, 8192], P('dp', 'tensor')
- normed: bfloat16 [16384, 8192], P('dp', 'tensor')
The draws below stay inside these ranges and needn't reach their ends.
Inputs may be any that keep to these rules, and one draw needn't show every extreme that they name: `image_grids`: each image is a grid of 3 to 8 rows by 2 to 8 columns of merged tokens; in every draw some image is 8 by 8. `routing`: each row names every offset 0 to 3 once.
All inputs are finite; a program needn't handle non-finite values.
Results may differ from the reference program's by a relative error of at most 0.006.
Values may be sent and summed in bfloat16 or wider, within the bound.
No kernel may reach another device: no remote copies, remote signals or barrier semaphores. Data moves between devices by JAX's collectives and lax.ppermute only.
A program may use at most 128 MiB of HBM per device.

```python
import jax
import jax.numpy as jnp
from jax import lax

D_VIT = 1280
D = 8192
D_MERGE = 5120
BLOCKS = 4
SLOTS = 256
CAP = 64
SEQ = 512
SHARDS = 32
PATCHES = 32768
TOTAL_SEQ = 16384
N_TENSOR = 4


def draw_patches(key, part):
    keys = jax.random.split(jax.random.fold_in(key, 11), 3)
    row_scale = jnp.exp(jax.random.uniform(keys[1], (PATCHES, 1), jnp.float32, jnp.log(0.5), jnp.log(5.0)))
    row_offset = jax.random.uniform(keys[2], (PATCHES, 1), jnp.float32, -1.0, 1.0)
    base = jax.random.normal(keys[0], (PATCHES, D_VIT), jnp.float32)
    base = jnp.clip(base, -5.0, 5.0)
    return (base * row_scale + row_offset).astype(jnp.bfloat16)


def draw_text_embeds(key, part):
    keys = jax.random.split(jax.random.fold_in(key, 23), 3)
    column_ids = jnp.arange(D, dtype=jnp.float32)
    column_scale = 0.6 * jnp.power(3.0, column_ids / (D - 1)) * jax.random.uniform(keys[1], (D,), jnp.float32, 0.7, 1.3)
    row_scale = jnp.exp(jax.random.uniform(keys[2], (TOTAL_SEQ, 1), jnp.float32, jnp.log(0.3), jnp.log(3.0)))
    base = jax.random.normal(keys[0], (TOTAL_SEQ, D), jnp.float32)
    base = jnp.clip(base, -5.0, 5.0)
    return (base * row_scale * column_scale[None, :]).astype(jnp.bfloat16)


def draw_image_grids(key, part):
    keys = jax.random.split(jax.random.fold_in(key, 37), 4)
    grid_rows = jax.random.randint(keys[0], (SHARDS, BLOCKS), 3, 9)
    grid_columns = jax.random.randint(keys[1], (SHARDS, BLOCKS), 2, CAP // 8 + 1)
    full_shard = jax.random.randint(keys[2], (), 0, SHARDS)
    full_block = jax.random.randint(keys[3], (), 0, BLOCKS)
    shard_ids = jnp.arange(SHARDS, dtype=jnp.int32)[:, None]
    block_ids = jnp.arange(BLOCKS, dtype=jnp.int32)[None, :]
    target = (shard_ids == full_shard) & (block_ids == full_block)
    grid_rows = jnp.where(target, 8, grid_rows)
    grid_columns = jnp.where(target, CAP // 8, grid_columns)
    return jnp.stack([grid_rows, grid_columns], axis=-1).astype(jnp.int32)


def levels(own_key, shape, pieces, smallest, largest):
    def one(dim, shards_of):
        steps = jax.random.uniform(jax.random.fold_in(jax.random.fold_in(own_key, 6), dim), (shards_of,), jnp.float32, smallest / len(pieces), largest / len(pieces))
        return jnp.repeat(jnp.exp(steps), shape[dim] // shards_of).reshape((-1,) + (1,) * (len(shape) - dim - 1))

    loudness = one(*pieces[0])
    for cut in pieces[1:]:
        loudness = loudness * one(*cut)
    return loudness


def normal_values(own_key, shape, width, most, cuts=(), kind=jnp.bfloat16):
    level = levels(own_key, shape, cuts, -0.22, 0.18) if cuts else 1.0
    drawn = jax.random.normal(own_key, shape, jnp.float32) * width * level
    return jnp.minimum(jnp.maximum(drawn, -most), most).astype(kind)


def setup_inputs(seed: int = 0) -> dict:
    seeds = jax.random.split(jax.random.key(seed), 12)
    patches = draw_patches(jax.random.fold_in(seeds[11], 71), 0)
    norm_gain = jnp.clip(1.0 + 0.18 * jax.random.normal(seeds[1], (D_VIT,), jnp.float32), 0.1, 1.9)
    norm_bias = normal_values(seeds[2], (D_VIT,), 0.5, 3.0, (), jnp.float32)
    first_weight = normal_values(seeds[3], (D_MERGE, D_MERGE), D_MERGE ** -0.5, 0.078125, ((1, 4),))
    first_bias = normal_values(seeds[4], (D_MERGE,), 0.5, 3.0, ((0, 4),), jnp.float32)
    second_weight = normal_values(seeds[5], (D_MERGE, D), D_MERGE ** -0.5, 0.078125, ((0, 4), (1, 32)))
    second_bias = normal_values(seeds[6], (D,), 0.3, 2.0, ((0, 4),), jnp.float32)
    text_embeds = draw_text_embeds(jax.random.fold_in(seeds[11], 71), 0)
    final_gain = jnp.clip(1.0 + 0.18 * jax.random.normal(seeds[8], (D,), jnp.float32), 0.1, 1.9)
    image_grids = draw_image_grids(jax.random.fold_in(seeds[11], 71), 0)
    routing = jax.vmap(lambda own: jax.random.permutation(own, BLOCKS))(jax.random.split(seeds[10], SHARDS)).reshape((SHARDS, BLOCKS)).astype(jnp.int32)
    return {"patches": patches, "norm_gain": norm_gain, "norm_bias": norm_bias, "first_weight": first_weight, "first_bias": first_bias, "second_weight": second_weight, "second_bias": second_bias, "text_embeds": text_embeds, "final_gain": final_gain, "image_grids": image_grids, "routing": routing}


def reference(patches, norm_gain, norm_bias, first_weight, first_bias, second_weight, second_bias, text_embeds, final_gain, image_grids, routing):
    patch_values = patches.astype(jnp.float32)
    centered = patch_values - lax.optimization_barrier(jnp.mean(patch_values, axis=-1, keepdims=True))
    variance = lax.optimization_barrier(jnp.mean(centered * centered, axis=-1, keepdims=True))
    normed_patches = centered * lax.rsqrt(variance + 1e-06) * norm_gain + norm_bias
    merged = normed_patches.reshape(-1, D_MERGE).astype(jnp.bfloat16)
    hidden = jax.nn.gelu(jnp.dot(merged, first_weight, preferred_element_type=jnp.float32) + first_bias, approximate=False).astype(jnp.bfloat16)
    group_width = D_MERGE // N_TENSOR
    summed = jnp.zeros((hidden.shape[0], D), jnp.float32)
    for group in range(N_TENSOR):
        partial_value = jnp.dot(hidden[:, group * group_width:(group + 1) * group_width], second_weight[group * group_width:(group + 1) * group_width], preferred_element_type=jnp.float32).astype(jnp.bfloat16)
        partial_value = lax.optimization_barrier(partial_value)
        summed = summed + partial_value.astype(jnp.float32)
    projected = (summed + second_bias).astype(jnp.bfloat16)
    counts_all = (image_grids[:, :, 0] * image_grids[:, :, 1]).astype(jnp.int32)
    shard_ids = jnp.arange(SHARDS, dtype=jnp.int32)[:, None]
    stride_ids = jnp.arange(BLOCKS, dtype=jnp.int32)[None, :]
    source_shard = ((shard_ids - stride_ids) % SHARDS).astype(jnp.int32)
    source_routing = routing[source_shard]
    block_ids = jnp.arange(BLOCKS, dtype=jnp.int32)[None, None, :]
    chosen = lax.optimization_barrier(jnp.sum(jnp.where(source_routing == stride_ids[:, :, None], block_ids, 0), axis=-1)).astype(jnp.int32)
    lengths = counts_all[source_shard, chosen]
    starts = (jnp.cumsum(lengths, axis=1) - lengths).astype(jnp.int32)
    totals = lax.optimization_barrier(jnp.sum(lengths, axis=1))
    position = jnp.arange(SEQ, dtype=jnp.int32)[None, :]
    which = lax.optimization_barrier(jnp.sum((position[:, :, None] >= starts[:, None, 1:]).astype(jnp.int32), axis=-1)).astype(jnp.int32)
    start_at = jnp.take_along_axis(starts, which, axis=1)
    source_at = jnp.take_along_axis(source_shard, which, axis=1)
    chosen_at = jnp.take_along_axis(chosen, which, axis=1)
    valid = position < totals[:, None]
    row_index = jnp.where(valid, source_at * SLOTS + chosen_at * CAP + position - start_at, 0).astype(jnp.int32)
    image_rows = jnp.take(projected, row_index.reshape(-1), axis=0).reshape(SHARDS, SEQ, D)
    text_rows = text_embeds.reshape(SHARDS, SEQ, D)
    embeddings = jnp.where(valid[:, :, None], image_rows, text_rows).reshape(SHARDS * SEQ, D)
    embed_values = embeddings.astype(jnp.float32)
    mean_square = lax.optimization_barrier(jnp.mean(embed_values * embed_values, axis=-1, keepdims=True))
    normed = (embed_values * lax.rsqrt(mean_square + 1e-06) * final_gain).astype(jnp.bfloat16)
    return (embeddings, normed)
```

```python
import itertools

import jax
import jax.numpy as jnp
import numpy as np
from jax import lax
from jax.experimental import pallas as pl
from jax.experimental.pallas import tpu as pltpu
from jax.sharding import Mesh, PartitionSpec as P

D = 8192
EPS = 1e-06
AXES = ("z", "y", "xl", "xh", "c")
SIZES = {"z": 4, "y": 4, "xl": 2, "xh": 2, "c": 2}
SHARDS = 32
BLOCKS = 4
CAP = 64
ROWS = BLOCKS * CAP
BF = jnp.bfloat16
F32 = jnp.float32
VMEM = pl.BlockSpec(memory_space=pltpu.VMEM)
SMEM = pl.BlockSpec(memory_space=pltpu.SMEM)
ANY = pl.BlockSpec(memory_space=pl.ANY)


def shift(value, **deltas):
    axes = tuple(a for a in AXES if a in deltas)
    sizes = [SIZES[a] for a in axes]
    pairs = []
    for src in itertools.product(*[range(s) for s in sizes]):
        dst = [(i + deltas[a]) % s for i, a, s in zip(src, axes, sizes)]
        pairs.append((int(np.ravel_multi_index(src, sizes)), int(np.ravel_multi_index(dst, sizes))))
    return lax.ppermute(value, axes, pairs)


def shift_dp(value, distance):
    pairs = [(i, (i + distance) % SHARDS) for i in range(SHARDS)]
    return lax.ppermute(value, ("z", "y", "xl"), pairs)


def place(idx_ref):
    i = idx_ref[0]
    return i >> 5, (i >> 3) & 3, (i >> 2) & 1, (i >> 1) & 1, i & 1, i >> 2


def block_of(routing_ref, shard, offset):
    block = jnp.int32(0)
    for b in range(1, BLOCKS):
        block = jnp.where(routing_ref[shard * BLOCKS + b] == offset, b, block)
    return block


def first_kernel(idx_ref, routing_ref, patches_ref, gain_ref, bias_ref, w_ref, b_ref, o0, o1, o2, o3, scr, merged):
    shard = place(idx_ref)[5]
    width = patches_ref.shape[1]

    @pl.when(pl.program_id(0) == 0)
    def _():
        for k in range(BLOCKS):
            block = block_of(routing_ref, shard, k)
            x = patches_ref[pl.ds(pl.multiple_of(block * ROWS, ROWS), ROWS), :].astype(F32)
            centered = x - jnp.mean(x, axis=-1, keepdims=True)
            variance = jnp.mean(centered * centered, axis=-1, keepdims=True)
            normed = centered * lax.rsqrt(variance + EPS) * gain_ref[...] + bias_ref[...]
            for t in range(width // 128):
                scr[t] = normed[:, t * 128 : (t + 1) * 128]
            for j in range(4):
                for t in range(width // 128):
                    at = j * width + t * 128
                    merged[k * CAP : (k + 1) * CAP, at : at + 128] = scr[t, pl.ds(j, CAP, stride=4), :].astype(BF)

    h = jnp.dot(merged[...], w_ref[...], preferred_element_type=F32) + b_ref[...]
    h = (0.5 * h * (1.0 + lax.erf(h * np.float32(np.sqrt(0.5))))).astype(BF)
    for k, o in enumerate((o0, o1, o2, o3)):
        o[...] = h[k * CAP : (k + 1) * CAP, :]


def first_product(idx, routing, patches, gain, bias, weight, bias1):
    depth, width = weight.shape
    cut = 256
    out = jax.ShapeDtypeStruct((CAP, width), BF)
    return pl.pallas_call(
        first_kernel,
        grid=(width // cut,),
        in_specs=[
            SMEM,
            SMEM,
            pl.BlockSpec(patches.shape, lambda n: (0, 0)),
            pl.BlockSpec((1, gain.shape[0]), lambda n: (0, 0)),
            pl.BlockSpec((1, gain.shape[0]), lambda n: (0, 0)),
            pl.BlockSpec((depth, cut), lambda n: (0, n)),
            pl.BlockSpec((1, cut), lambda n: (0, n)),
        ],
        out_specs=[pl.BlockSpec((CAP, cut), lambda n: (0, n))] * BLOCKS,
        out_shape=[out] * BLOCKS,
        scratch_shapes=[pltpu.VMEM((patches.shape[1] // 128, ROWS, 128), F32), pltpu.VMEM((ROWS, depth), BF)],
        compiler_params=pltpu.CompilerParams(vmem_limit_bytes=40 << 20),
        name="first_product",
    )(idx, routing, patches, gain[None], bias[None], weight, bias1[None])


CHUNKS = tuple((dz, dx) for dz in range(4) for dx in range(2))


def second_kernel(idx_ref, *refs):
    rows = refs[:2]
    weights = refs[2:10]
    keep, send = refs[10:]
    z, y, xl, xh, c, _ = place(idx_ref)
    for (dz, dx), w in zip(CHUNKS, weights):
        group = (z - dz) & 3
        column = pl.multiple_of((xl ^ dx) * 256, 256)
        side = (group >> 1) ^ xh
        other = (group & 1) ^ c
        values = [jnp.dot(r[...], w[...], preferred_element_type=F32).astype(BF) for r in rows]

        @pl.when(other == 0)
        def _():
            for i, v in enumerate(values):
                keep[side, i * ROWS : (i + 1) * ROWS, pl.ds(column, 256)] = v

        @pl.when(other == 1)
        def _():
            for i, v in enumerate(values):
                send[side, i * ROWS : (i + 1) * ROWS, pl.ds(column, 256)] = v


def second_product(idx, rows, weights, name):
    out = jax.ShapeDtypeStruct((2, 2 * ROWS, 512), BF)
    return pl.pallas_call(
        second_kernel,
        in_specs=[SMEM] + [VMEM] * 10,
        out_specs=[VMEM, VMEM],
        out_shape=[out, out],
        compiler_params=pltpu.CompilerParams(vmem_limit_bytes=40 << 20),
        name=name,
    )(idx, *rows, *weights)


def row_sums(v):
    ones = jnp.ones((8, v.shape[1]), F32)
    return lax.dot_general(ones, v * v, (((1,), (1,)), ((), ())), precision=lax.Precision.HIGHEST, preferred_element_type=F32)


def text_kernel(text_ref, out_ref, sum_ref):
    value = text_ref[...]
    out_ref[...] = value
    sum_ref[...] = row_sums(value.astype(F32))


def splice_kernel(idx_ref, routing_ref, grids_ref, *refs):
    stay = refs[:4]
    cross = refs[4:8]
    bias_ref, text_ref, _, out_ref, sum_ref = refs[8:]
    z, y, xl, xh, c, shard = place(idx_ref)
    row = lax.broadcasted_iota(jnp.int32, (ROWS, CAP), 0)
    col = lax.broadcasted_iota(jnp.int32, (ROWS, CAP), 1)
    filled = jnp.int32(0)
    picks = []
    for k in range(BLOCKS):
        source = (shard - k) & (SHARDS - 1)
        block = block_of(routing_ref, source, k)
        at = (source * BLOCKS + block) * 2
        count = grids_ref[at] * grids_ref[at + 1]
        picks.append(jnp.where((row == col + filled) & (col < count), 1.0, 0.0))
        filled = filled + count
    pick = jnp.concatenate(picks, axis=1).astype(BF)
    live = lax.broadcasted_iota(jnp.int32, (ROWS, 512), 0) < filled
    total = jnp.zeros((8, ROWS), F32)
    for j in range(4):
        column = pl.multiple_of(((y + j) & 3) * 512, 512)
        value = stay[j][...].astype(F32) + cross[j][...].astype(F32) + bias_ref[:, pl.ds(column, 512)]
        image = jnp.dot(pick, value.astype(BF), preferred_element_type=F32)
        text = text_ref[:, pl.ds(column, 512)]
        value = jnp.where(live, image, text.astype(F32))
        out_ref[:, pl.ds(column, 512)] = value.astype(BF)
        total = total + row_sums(value)
    sum_ref[...] = total


def norm_kernel(emb_ref, sum_ref, gain_ref, *refs):
    out_ref = refs[-1]
    scale = lax.rsqrt(sum_ref[...] / D + EPS).T[:, :1]
    out_ref[...] = (emb_ref[...].astype(F32) * scale * gain_ref[...]).astype(BF)


def half(width, which):
    return pl.BlockSpec((ROWS, width), lambda i: (which, 0))


def whole(shape):
    return pl.BlockSpec(shape, lambda i: (0,) * len(shape))


def text_half(text):
    rows, width = text.shape
    return pl.pallas_call(
        text_kernel,
        grid=(1,),
        in_specs=[half(width, 1)],
        out_specs=[half(width, 1), whole((8, ROWS))],
        out_shape=[jax.ShapeDtypeStruct(text.shape, BF), jax.ShapeDtypeStruct((8, ROWS), F32)],
        name="text_half",
    )(text)


def splice(idx, routing, grids, stay, cross, bias, text, emb):
    rows, width = text.shape
    piece = whole((ROWS, 512))
    return pl.pallas_call(
        splice_kernel,
        grid=(1,),
        in_specs=[SMEM] * 3 + [piece] * 8 + [whole((1, width)), half(width, 0), ANY],
        out_specs=[half(width, 0), whole((8, ROWS))],
        out_shape=[jax.ShapeDtypeStruct(text.shape, BF), jax.ShapeDtypeStruct((8, ROWS), F32)],
        input_output_aliases={13: 0},
        name="splice",
    )(idx, routing, grids, *stay, *cross, bias[None], text, emb)


def norm_half(emb, sums, gain, which, base=None):
    rows, width = emb.shape
    args = [emb, sums, gain[None]]
    specs = [half(width, which), whole((8, ROWS)), whole((1, width))]
    alias = {}
    if base is not None:
        args.append(base)
        specs.append(ANY)
        alias = {3: 0}
    return pl.pallas_call(
        norm_kernel,
        grid=(1,),
        in_specs=specs,
        out_specs=half(width, which),
        out_shape=jax.ShapeDtypeStruct(emb.shape, BF),
        input_output_aliases=alias,
        name="norm_half",
    )(*args)


def over_tensor(sums):
    sums = sums + shift(sums, c=1)
    return sums + shift(sums, xh=1)


def per_device(
    patches,
    norm_gain,
    norm_bias,
    first_weight,
    first_bias,
    second_weight,
    second_bias,
    text_embeds,
    final_gain,
    image_grids,
    routing,
):
    idx = lax.axis_index(AXES).astype(jnp.int32).reshape(1)
    routing = routing.reshape(-1)
    grids = image_grids.reshape(-1)

    weights = {(0, 0): second_weight}
    for dz, dx in ((1, 1), (3, 1), (2, 1)):
        weights[dz, dx] = shift(second_weight, z=dz, xl=dx)
    blocks = first_product(idx, routing, patches, norm_gain, norm_bias, first_weight, first_bias)
    blocks = [blocks[0]] + [shift_dp(blocks[k], k) for k in range(1, BLOCKS)]
    rest, blocks[0] = lax.optimization_barrier((second_weight, blocks[0]))
    for dz, dx in ((0, 1), (1, 0), (3, 0), (2, 0)):
        weights[dz, dx] = shift(rest, z=dz, xl=dx)
    weights = [weights[chunk] for chunk in CHUNKS]
    own = jnp.concatenate(blocks, axis=0)
    rows = {0: own}
    for j in (1, 3, 2):
        rows[j] = shift(own, y=j)

    stay, cross = {}, {}
    for pair, name in (((1, 3), "second_a"), ((2, 0), "second_b")):
        keep, send = second_product(idx, [rows[j] for j in pair], weights, name)
        came = shift(send, c=1)
        for side, taken in ((1, cross), (0, stay)):
            for i, j in enumerate(pair):
                at = slice(i * ROWS, (i + 1) * ROWS)
                piece = (keep[side, at].astype(F32) + came[side, at].astype(F32)).astype(BF)
                if side:
                    taken[j] = shift(piece, y=-j % 4, xh=1)
                elif j:
                    taken[j] = shift(piece, y=-j % 4)
                else:
                    taken[j] = piece

    emb, text_sums = text_half(text_embeds)
    normed = norm_half(emb, over_tensor(text_sums), final_gain, 1)
    emb, sums = splice(
        idx, routing, grids, [stay[j] for j in range(4)], [cross[j] for j in range(4)], second_bias, text_embeds, emb
    )
    normed = norm_half(emb, over_tensor(sums), final_gain, 0, normed)
    return (emb, normed)


def solution(mesh):
    mesh = Mesh(mesh.devices.reshape([SIZES[a] for a in AXES]), AXES)
    dp, tensor = ("z", "y", "xl"), ("xh", "c")
    placed = (
        P(dp, None),
        P(),
        P(),
        P(None, tensor),
        P(tensor),
        P(tensor, dp),
        P(tensor),
        P(dp, tensor),
        P(tensor),
        P(),
        P(),
    )
    return jax.shard_map(
        per_device,
        mesh=mesh,
        in_specs=placed,
        out_specs=(P(dp, tensor), P(dp, tensor)),
        check_vma=False,
    )
```

```python
import itertools

import jax
import jax.numpy as jnp
import numpy as np
from jax import lax
from jax.experimental import pallas as pl
from jax.experimental.pallas import tpu as pltpu
from jax.sharding import Mesh, PartitionSpec as P


D = 8192
EPS = 1e-06
AXES = ("z", "y", "xl", "xh", "c")
SIZES = {"z": 4, "y": 4, "xl": 2, "xh": 2, "c": 2}
SHARDS = 32
BLOCKS = 4
CAP = 64
ROWS = BLOCKS * CAP
BF = jnp.bfloat16
F32 = jnp.float32
VMEM = pl.BlockSpec(memory_space=pltpu.VMEM)
SMEM = pl.BlockSpec(memory_space=pltpu.SMEM)
ANY = pl.BlockSpec(memory_space=pl.ANY)


def shift(value, **deltas):
    axes = tuple(a for a in AXES if a in deltas)
    sizes = [SIZES[a] for a in axes]
    pairs = []
    for src in itertools.product(*[range(s) for s in sizes]):
        dst = [(i + deltas[a]) % s for i, a, s in zip(src, axes, sizes)]
        pairs.append((int(np.ravel_multi_index(src, sizes)), int(np.ravel_multi_index(dst, sizes))))
    return lax.ppermute(value, axes, pairs)


def shift_dp(value, distance):
    pairs = [(i, (i + distance) % SHARDS) for i in range(SHARDS)]
    return lax.ppermute(value, ("z", "y", "xl"), pairs)


def place(idx_ref):
    i = idx_ref[0]
    return i >> 5, (i >> 3) & 3, (i >> 2) & 1, (i >> 1) & 1, i & 1, i >> 2


def block_of(routing_ref, shard, offset):
    block = jnp.int32(0)
    for b in range(1, BLOCKS):
        block = jnp.where(routing_ref[shard, b] == offset, b, block)
    return block


def first_kernel(idx_ref, routing_ref, patches_ref, gain_ref, bias_ref, w_ref, b_ref, o0, o1, o2, o3, raw, scr, merged, sems):
    shard = place(idx_ref)[5]
    width = patches_ref.shape[1]
    cut = w_ref.shape[1]
    step = pl.program_id(0)

    def fetch(k):
        block = block_of(routing_ref, shard, k)
        rows = pl.ds(pl.multiple_of(block * ROWS, ROWS), ROWS)
        return pltpu.make_async_copy(patches_ref.at[rows, :], raw.at[k], sems.at[k])

    @pl.when(step == 0)
    def _():
        for k in range(BLOCKS):
            fetch(k).start()
        for k in range(BLOCKS):
            fetch(k).wait()
            x = raw[k].astype(F32)
            centered = x - jnp.mean(x, axis=-1, keepdims=True)
            variance = jnp.mean(centered * centered, axis=-1, keepdims=True)
            normed = centered * lax.rsqrt(variance + EPS) * gain_ref[...][None] + bias_ref[...][None]
            for t in range(width // 128):
                scr[t] = normed[:, t * 128 : (t + 1) * 128]
            for j in range(4):
                for t in range(width // 128):
                    at = j * width + t * 128
                    merged[k * CAP : (k + 1) * CAP, at : at + 128] = scr[t, pl.ds(j, CAP, stride=4), :].astype(BF)

    h = jnp.dot(merged[...], w_ref[...], preferred_element_type=F32)
    h = h + b_ref[pl.ds(pl.multiple_of(step * cut, cut), cut)][None]
    h = (0.5 * h * (1.0 + lax.erf(h * np.float32(np.sqrt(0.5))))).astype(BF)
    for k, o in enumerate((o0, o1, o2, o3)):
        o[...] = h[k * CAP : (k + 1) * CAP, :]


def first_product(idx, routing, patches, gain, bias, weight, bias1):
    depth, width = weight.shape
    cut = 256
    out = jax.ShapeDtypeStruct((CAP, width), BF)
    return pl.pallas_call(
        first_kernel,
        grid=(width // cut,),
        in_specs=[SMEM, SMEM, ANY, VMEM, VMEM, pl.BlockSpec((depth, cut), lambda n: (0, n)), VMEM],
        out_specs=[pl.BlockSpec((CAP, cut), lambda n: (0, n))] * BLOCKS,
        out_shape=[out] * BLOCKS,
        scratch_shapes=[
            pltpu.VMEM((BLOCKS, ROWS, patches.shape[1]), BF),
            pltpu.VMEM((patches.shape[1] // 128, ROWS, 128), F32),
            pltpu.VMEM((ROWS, depth), BF),
            pltpu.SemaphoreType.DMA((BLOCKS,)),
        ],
        compiler_params=pltpu.CompilerParams(vmem_limit_bytes=40 << 20),
        name="first_product",
    )(idx, routing, patches, gain, bias, weight, bias1)


CHUNKS = tuple((dz, dx) for dz in range(4) for dx in range(2))


def second_kernel(idx_ref, *refs):
    pieces = refs[:4]
    weights = refs[4:12]
    keep, send, rows = refs[12:]
    z, _, xl, xh, c, _ = place(idx_ref)
    for i in range(2):
        rows[i * ROWS : i * ROWS + CAP, :] = pieces[2 * i][...]
        rows[i * ROWS + CAP : (i + 1) * ROWS, :] = pieces[2 * i + 1][...]
    for (dz, dx), w in zip(CHUNKS, weights):
        group = (z - dz) & 3
        column = pl.multiple_of((xl ^ dx) * 256, 256)
        side = (group >> 1) ^ xh
        other = (group & 1) ^ c
        values = [
            jnp.dot(rows[i * ROWS : (i + 1) * ROWS, :], w[...], preferred_element_type=F32).astype(BF) for i in range(2)
        ]

        @pl.when(other == 0)
        def _():
            for i, v in enumerate(values):
                keep[side, i * ROWS : (i + 1) * ROWS, pl.ds(column, 256)] = v

        @pl.when(other == 1)
        def _():
            for i, v in enumerate(values):
                send[side, i * ROWS : (i + 1) * ROWS, pl.ds(column, 256)] = v


def second_product(idx, pieces, weights):
    out = jax.ShapeDtypeStruct((2, 2 * ROWS, 512), BF)
    return pl.pallas_call(
        second_kernel,
        in_specs=[SMEM] + [VMEM] * 12,
        out_specs=[VMEM, VMEM],
        out_shape=[out, out],
        scratch_shapes=[pltpu.VMEM((2 * ROWS, weights[0].shape[0]), BF)],
        compiler_params=pltpu.CompilerParams(vmem_limit_bytes=40 << 20),
    )(idx, *pieces, *weights)


def row_sums(v):
    ones = jnp.ones((8, v.shape[1]), F32)
    return lax.dot_general(ones, v * v, (((1,), (1,)), ((), ())), precision=lax.Precision.HIGHEST, preferred_element_type=F32)


def text_kernel(text_ref, out_ref, sum_ref):
    value = text_ref[...]
    out_ref[...] = value
    sum_ref[...] = row_sums(value.astype(F32))


def splice_kernel(idx_ref, routing_ref, grids_ref, *refs):
    stay = refs[:4]
    cross = refs[4:8]
    bias_ref, text_ref, _, out_ref, sum_ref = refs[8:]
    _, y, _, _, _, shard = place(idx_ref)
    row = lax.broadcasted_iota(jnp.int32, (ROWS, CAP), 0)
    col = lax.broadcasted_iota(jnp.int32, (ROWS, CAP), 1)
    filled = jnp.int32(0)
    picks = []
    for k in range(BLOCKS):
        source = (shard - k) & (SHARDS - 1)
        block = block_of(routing_ref, source, k)
        count = grids_ref[source, 2 * block] * grids_ref[source, 2 * block + 1]
        picks.append(jnp.where((row == col + filled) & (col < count), 1.0, 0.0))
        filled = filled + count
    pick = jnp.concatenate(picks, axis=1).astype(BF)
    live = lax.broadcasted_iota(jnp.int32, (ROWS, 512), 0) < filled
    total = jnp.zeros((8, ROWS), F32)
    for j in range(4):
        column = pl.multiple_of(((y + j) & 3) * 512, 512)
        value = stay[j][...].astype(F32) + cross[j][...].astype(F32) + bias_ref[pl.ds(column, 512)][None]
        image = jnp.dot(pick, value.astype(BF), preferred_element_type=F32)
        text = text_ref[:, pl.ds(column, 512)]
        value = jnp.where(live, image, text.astype(F32))
        out_ref[:, pl.ds(column, 512)] = value.astype(BF)
        total = total + row_sums(value)
    sum_ref[...] = total


def norm_kernel(emb_ref, s0, s1, s2, s3, gain_ref, *refs):
    out_ref = refs[-1]
    total = s0[...] + s1[...] + s2[...] + s3[...]
    scale = lax.rsqrt(total / D + EPS).T[:, :1]
    out_ref[...] = (emb_ref[...].astype(F32) * scale * gain_ref[...][None]).astype(BF)


def half(width, which):
    return pl.BlockSpec((ROWS, width), lambda i: (which, 0))


def whole(shape):
    return pl.BlockSpec(shape, lambda i: (0,) * len(shape))


def text_half(text):
    _, width = text.shape
    return pl.pallas_call(
        text_kernel,
        grid=(1,),
        in_specs=[half(width, 1)],
        out_specs=[half(width, 1), whole((8, ROWS))],
        out_shape=[jax.ShapeDtypeStruct(text.shape, BF), jax.ShapeDtypeStruct((8, ROWS), F32)],
        name="text_half",
    )(text)


def splice(idx, routing, grids, stay, cross, bias, text, emb):
    _, width = text.shape
    piece = whole((ROWS, 512))
    return pl.pallas_call(
        splice_kernel,
        grid=(1,),
        in_specs=[SMEM] * 3 + [piece] * 8 + [whole((width,)), half(width, 0), ANY],
        out_specs=[half(width, 0), whole((8, ROWS))],
        out_shape=[jax.ShapeDtypeStruct(text.shape, BF), jax.ShapeDtypeStruct((8, ROWS), F32)],
        input_output_aliases={13: 0},
        name="splice",
    )(idx, routing, grids, *stay, *cross, bias, text, emb)


def norm_half(emb, sums, gain, which, base=None):
    _, width = emb.shape
    args = [emb, *sums, gain]
    specs = [half(width, which)] + [whole((8, ROWS))] * 4 + [whole((width,))]
    alias = {}
    if base is not None:
        args.append(base)
        specs.append(ANY)
        alias = {6: 0}
    return pl.pallas_call(
        norm_kernel,
        grid=(1,),
        in_specs=specs,
        out_specs=half(width, which),
        out_shape=jax.ShapeDtypeStruct(emb.shape, BF),
        input_output_aliases=alias,
    )(*args)


def over_tensor(sums):
    across = shift(sums, xh=1)
    return [sums, shift(sums, c=1), across, shift(across, c=1)]


def per_device(
    patches,
    norm_gain,
    norm_bias,
    first_weight,
    first_bias,
    second_weight,
    second_bias,
    text_embeds,
    final_gain,
    image_grids,
    routing,
):
    idx = lax.axis_index(AXES).astype(jnp.int32).reshape(1)
    grids = image_grids.reshape(image_grids.shape[0], -1)

    weights = {(0, 0): second_weight}
    weights[0, 1] = shift(second_weight, xl=1)
    weights[1, 0] = shift(second_weight, z=1)
    weights[3, 0] = shift(second_weight, z=3)
    weights[1, 1] = shift(weights[0, 1], z=1)
    weights[3, 1] = shift(weights[0, 1], z=3)
    weights[2, 0] = shift(weights[1, 0], z=1)
    weights[2, 1] = shift(weights[3, 1], z=3)
    weights = [weights[chunk] for chunk in CHUNKS]

    blocks = first_product(idx, routing, patches, norm_gain, norm_bias, first_weight, first_bias)
    head = {0: blocks[0]}
    tail = {0: jnp.concatenate([shift_dp(blocks[k], k) for k in range(1, BLOCKS)], axis=0)}
    for j in (1, 3, 2):
        head[j] = shift(head[0], y=j)
        tail[j] = shift(tail[0], y=j)

    stay, cross = {}, {}
    for pair in ((1, 3), (2, 0)):
        pieces = [part[j] for j in pair for part in (head, tail)]
        keep, send = second_product(idx, pieces, weights)
        came = shift(send, c=1)
        for side, taken in ((1, cross), (0, stay)):
            for i, j in enumerate(pair):
                at = slice(i * ROWS, (i + 1) * ROWS)
                piece = (keep[side, at].astype(F32) + came[side, at].astype(F32)).astype(BF)
                if side:
                    taken[j] = shift(piece, y=-j % 4, xh=1)
                elif j:
                    taken[j] = shift(piece, y=-j % 4)
                else:
                    taken[j] = piece

    emb, text_sums = text_half(text_embeds)
    normed = norm_half(emb, over_tensor(text_sums), final_gain, 1)
    emb, sums = splice(
        idx, routing, grids, [stay[j] for j in range(4)], [cross[j] for j in range(4)], second_bias, text_embeds, emb
    )
    normed = norm_half(emb, over_tensor(sums), final_gain, 0, normed)
    return (emb, normed)


def solution(mesh):
    mesh = Mesh(mesh.devices.reshape([SIZES[a] for a in AXES]), AXES)
    dp, tensor = ("z", "y", "xl"), ("xh", "c")
    placed = (
        P(dp, None),
        P(),
        P(),
        P(None, tensor),
        P(tensor),
        P(tensor, dp),
        P(tensor),
        P(dp, tensor),
        P(tensor),
        P(),
        P(),
    )
    return jax.shard_map(
        per_device,
        mesh=mesh,
        in_specs=placed,
        out_specs=(P(dp, tensor), P(dp, tensor)),
        check_vma=False,
    )
```

```python
import itertools

import jax
import jax.numpy as jnp
import numpy as np
from jax import lax
from jax.experimental import pallas as pl
from jax.experimental.pallas import tpu as pltpu
from jax.sharding import Mesh, PartitionSpec as P


D = 8192
EPS = 1e-06
AXES = ("z", "y", "xl", "xh", "c")
SIZES = {"z": 4, "y": 4, "xl": 2, "xh": 2, "c": 2}
SHARDS = 32
BLOCKS = 4
CAP = 64
ROWS = BLOCKS * CAP
BF = jnp.bfloat16
F32 = jnp.float32
VMEM = pl.BlockSpec(memory_space=pltpu.VMEM)
SMEM = pl.BlockSpec(memory_space=pltpu.SMEM)
ANY = pl.BlockSpec(memory_space=pl.ANY)


def shift(value, **deltas):
    axes = tuple(a for a in AXES if a in deltas)
    sizes = [SIZES[a] for a in axes]
    pairs = []
    for src in itertools.product(*[range(s) for s in sizes]):
        dst = [(i + deltas[a]) % s for i, a, s in zip(src, axes, sizes)]
        pairs.append((int(np.ravel_multi_index(src, sizes)), int(np.ravel_multi_index(dst, sizes))))
    return lax.ppermute(value, axes, pairs)


def shift_dp(value, distance):
    pairs = [(i, (i + distance) % SHARDS) for i in range(SHARDS)]
    return lax.ppermute(value, ("z", "y", "xl"), pairs)


def place(idx_ref):
    i = idx_ref[0]
    return i >> 5, (i >> 3) & 3, (i >> 2) & 1, (i >> 1) & 1, i & 1, i >> 2


def block_of(routing_ref, shard, offset):
    block = jnp.int32(0)
    for b in range(1, BLOCKS):
        block = jnp.where(routing_ref[b, shard] == offset, b, block)
    return block


def first_kernel(idx_ref, routing_ref, patches_ref, gain_hbm, bias_hbm, w_hbm, b_hbm, *refs):
    outs = refs[:BLOCKS]
    raw, scr, merged, wide, acc, gain_ref, bias_ref, b_ref, sems = refs[BLOCKS:]
    shard = place(idx_ref)[5]
    width = patches_ref.shape[1]
    tiles = width // 128
    cuts = [slice(n, n + 256) for n in range(0, w_hbm.shape[1], 256)]

    copies = []
    for small, held in ((gain_hbm, gain_ref), (bias_hbm, bias_ref)):
        copies.append(pltpu.make_async_copy(small, held, sems.at[len(copies)]))
    for k in range(BLOCKS):
        rows = pl.ds(pl.multiple_of(block_of(routing_ref, shard, k) * ROWS, ROWS), ROWS)
        copies.append(pltpu.make_async_copy(patches_ref.at[rows, :], raw.at[k], sems.at[len(copies)]))
    for j in range(4):
        copies.append(pltpu.make_async_copy(w_hbm.at[pl.ds(j * width, width), :], wide.at[j], sems.at[len(copies)]))
    copies.append(pltpu.make_async_copy(b_hbm, b_ref, sems.at[len(copies)]))
    for copy in copies:
        copy.start()
    for copy in copies[:2]:
        copy.wait()
    for k in range(BLOCKS):
        copies[2 + k].wait()
        for t in range(tiles):
            scr[k, t] = raw[k, :, t * 128 : (t + 1) * 128].astype(F32)

    def normalize(j):
        for k in range(BLOCKS):
            for half in range(2):
                x = [scr[k, t, pl.ds(j + 128 * half, 32, stride=4), :] for t in range(tiles)]
                mean = jnp.sum(sum(x), axis=-1, keepdims=True) / width
                x = [v - mean for v in x]
                variance = jnp.sum(sum(v * v for v in x), axis=-1, keepdims=True) / width
                scale = lax.rsqrt(variance + EPS)
                at = slice(k * CAP + half * 32, k * CAP + half * 32 + 32)
                for t, v in enumerate(x):
                    lanes = slice(t * 128, (t + 1) * 128)
                    merged[j, at, lanes] = (v * scale * gain_ref[lanes][None] + bias_ref[lanes][None]).astype(BF)

    normalize(0)
    for j in range(4):
        copies[2 + BLOCKS + j].wait()
        if j < 3:
            normalize(j + 1)
        else:
            copies[-1].wait()
        for cut in cuts:
            part = jnp.dot(merged[j], wide[j, :, cut], preferred_element_type=F32)
            if j == 0:
                acc[:, cut] = part
            elif j < 3:
                acc[:, cut] += part
            else:
                h = acc[:, cut] + part + b_ref[cut][None]
                h = (0.5 * h * (1.0 + lax.erf(h * np.float32(np.sqrt(0.5))))).astype(BF)
                for k, o in enumerate(outs):
                    o[:, cut] = h[k * CAP : (k + 1) * CAP, :]


def first_product(idx, routing, patches, gain, bias, weight, bias1):
    _, width = weight.shape
    vit = patches.shape[1]
    return pl.pallas_call(
        first_kernel,
        in_specs=[SMEM, SMEM] + [ANY] * 5,
        out_specs=[VMEM] * BLOCKS,
        out_shape=[jax.ShapeDtypeStruct((CAP, width), BF)] * BLOCKS,
        scratch_shapes=[
            pltpu.VMEM((BLOCKS, ROWS, vit), BF),
            pltpu.VMEM((BLOCKS, vit // 128, ROWS, 128), F32),
            pltpu.VMEM((4, ROWS, vit), BF),
            pltpu.VMEM((4, vit, width), BF),
            pltpu.VMEM((ROWS, width), F32),
            pltpu.VMEM(gain.shape, F32),
            pltpu.VMEM(bias.shape, F32),
            pltpu.VMEM(bias1.shape, F32),
            pltpu.SemaphoreType.DMA((7 + BLOCKS,)),
        ],
        compiler_params=pltpu.CompilerParams(vmem_limit_bytes=48 << 20),
        name="first_product",
    )(idx, routing, patches, gain, bias, weight, bias1)


CHUNKS = tuple((dz, dx) for dz in range(4) for dx in range(2))


def each_chunk(idx_ref, weights, wanted, use):
    z, _, xl, xh, c, _ = place(idx_ref)
    for (dz, dx), w in zip(CHUNKS, weights):
        group = (z - dz) & 3
        column = pl.ds(pl.multiple_of((xl ^ dx) * 256, 256), 256)
        side = (group >> 1) ^ xh

        @pl.when((group & 1) ^ c == wanted)
        def _():
            use(side, column, w)


def product(rows, i, w):
    return jnp.dot(rows[i * ROWS : (i + 1) * ROWS, :], w[...], preferred_element_type=F32)


def send_kernel(idx_ref, *refs):
    pieces = refs[:4]
    send, rows = refs[12:]
    for i in range(2):
        rows[i * ROWS : i * ROWS + CAP, :] = pieces[2 * i][...]
        rows[i * ROWS + CAP : (i + 1) * ROWS, :] = pieces[2 * i + 1][...]

    def use(side, column, w):
        for i in range(2):
            send[side, i * ROWS : (i + 1) * ROWS, column] = product(rows, i, w).astype(BF)

    each_chunk(idx_ref, refs[4:12], 1, use)


def keep_kernel(idx_ref, rows, came, *refs):
    outs = refs[8:]
    split = len(outs) == 4

    def use(side, column, w):
        values = []
        for i in range(2):
            at = slice(i * ROWS, (i + 1) * ROWS)
            values.append((product(rows, i, w) + came[side, at, column].astype(F32)).astype(BF))
        for s in range(2):

            @pl.when(side == s)
            def _():
                for i, v in enumerate(values):
                    if split:
                        outs[2 * s + i][:, column] = v
                    else:
                        outs[s][i * ROWS : (i + 1) * ROWS, column] = v

    each_chunk(idx_ref, refs[:8], 0, use)


def send_product(idx, pieces, weights):
    depth = weights[0].shape[0]
    return pl.pallas_call(
        send_kernel,
        in_specs=[SMEM] + [VMEM] * 12,
        out_specs=[VMEM, VMEM],
        out_shape=[jax.ShapeDtypeStruct((2, 2 * ROWS, 512), BF), jax.ShapeDtypeStruct((2 * ROWS, depth), BF)],
        compiler_params=pltpu.CompilerParams(vmem_limit_bytes=40 << 20),
    )(idx, *pieces, *weights)


def keep_product(idx, rows, came, weights, split):
    height, number = (ROWS, 4) if split else (2 * ROWS, 2)
    return pl.pallas_call(
        keep_kernel,
        in_specs=[SMEM] + [VMEM] * 10,
        out_specs=[VMEM] * number,
        out_shape=[jax.ShapeDtypeStruct((height, 512), BF)] * number,
        compiler_params=pltpu.CompilerParams(vmem_limit_bytes=40 << 20),
    )(idx, rows, came, *weights)


def lane_sums(v):
    v = v * v
    return sum(v[:, i : i + 128] for i in range(0, v.shape[1], 128))


def row_sums(v):
    ones = jnp.ones((8, v.shape[1]), F32)
    return lax.dot_general(ones, v, (((1,), (1,)), ((), ())), precision=lax.Precision.HIGHEST, preferred_element_type=F32)


def text_kernel(text_ref, out_ref, sum_ref):
    value = text_ref[...]
    out_ref[...] = value
    sum_ref[...] = row_sums(lane_sums(value.astype(F32)))


def splice_kernel(idx_ref, routing_ref, grids_ref, *refs):
    pieces = [[refs[0], refs[1]], [refs[2]], [refs[3], refs[4]], [refs[5]]]
    bias_ref, text_ref, _, out_ref, sum_ref = refs[6:]
    _, y, _, _, _, shard = place(idx_ref)
    row = lax.broadcasted_iota(jnp.int32, (ROWS, CAP), 0)
    col = lax.broadcasted_iota(jnp.int32, (ROWS, CAP), 1)
    filled = jnp.int32(0)
    picks = []
    for k in range(BLOCKS):
        source = (shard - k) & (SHARDS - 1)
        block = block_of(routing_ref, source, k)
        count = grids_ref[block, 0, source] * grids_ref[block, 1, source]
        picks.append(jnp.where((row == col + filled) & (col < count), 1.0, 0.0))
        filled = filled + count
    pick = jnp.concatenate(picks, axis=1).astype(BF)
    live = lax.broadcasted_iota(jnp.int32, (ROWS, 512), 0) < filled
    total = jnp.zeros((ROWS, 128), F32)
    for j in range(4):
        column = pl.ds(pl.multiple_of(((y + j) & 3) * 512, 512), 512)
        value = bias_ref[column][None] + sum(p[...].astype(F32) for p in pieces[j])
        image = jnp.dot(pick, value.astype(BF), preferred_element_type=F32)
        value = jnp.where(live, image, text_ref[:, column].astype(F32))
        out_ref[:, column] = value.astype(BF)
        total = total + lane_sums(value)
    sum_ref[...] = row_sums(total)


def norm_kernel(emb_ref, s0, s1, s2, s3, gain_ref, *refs):
    out_ref = refs[-1]
    total = s0[...] + s1[...] + s2[...] + s3[...]
    scale = lax.rsqrt(total / D + EPS).T[:, :1]
    out_ref[...] = (emb_ref[...].astype(F32) * scale * gain_ref[...][None]).astype(BF)


def half(width, which):
    return pl.BlockSpec((ROWS, width), lambda i: (which, 0))


def whole(shape):
    return pl.BlockSpec(shape, lambda i: (0,) * len(shape))


def text_half(text):
    _, width = text.shape
    return pl.pallas_call(
        text_kernel,
        grid=(1,),
        in_specs=[half(width, 1)],
        out_specs=[half(width, 1), whole((8, ROWS))],
        out_shape=[jax.ShapeDtypeStruct(text.shape, BF), jax.ShapeDtypeStruct((8, ROWS), F32)],
        name="text_half",
    )(text)


def splice(idx, routing, grids, pieces, bias, text, emb):
    _, width = text.shape
    return pl.pallas_call(
        splice_kernel,
        grid=(1,),
        in_specs=[SMEM] * 3 + [VMEM] * len(pieces) + [whole((width,)), half(width, 0), ANY],
        out_specs=[half(width, 0), whole((8, ROWS))],
        out_shape=[jax.ShapeDtypeStruct(text.shape, BF), jax.ShapeDtypeStruct((8, ROWS), F32)],
        input_output_aliases={5 + len(pieces): 0},
        name="splice",
    )(idx, routing, grids, *pieces, bias, text, emb)


def norm_half(emb, sums, gain, which, base=None):
    _, width = emb.shape
    args = [emb, *sums, gain]
    specs = [half(width, which)] + [whole((8, ROWS))] * 4 + [whole((width,))]
    alias = {}
    if base is not None:
        args.append(base)
        specs.append(ANY)
        alias = {6: 0}
    return pl.pallas_call(
        norm_kernel,
        grid=(1,),
        in_specs=specs,
        out_specs=half(width, which),
        out_shape=jax.ShapeDtypeStruct(emb.shape, BF),
        input_output_aliases=alias,
    )(*args)


def over_tensor(sums):
    across = shift(sums, xh=1)
    return [sums, shift(sums, c=1), across, shift(across, c=1)]


def per_device(
    patches,
    norm_gain,
    norm_bias,
    first_weight,
    first_bias,
    second_weight,
    second_bias,
    text_embeds,
    final_gain,
    image_grids,
    routing,
):
    idx = lax.axis_index(AXES).astype(jnp.int32).reshape(1)
    routing = routing.T
    grids = jnp.transpose(image_grids, (1, 2, 0))

    weights = {(0, 0): second_weight}
    weights[0, 1] = shift(second_weight, xl=1)
    weights[1, 0] = shift(second_weight, z=1)
    weights[3, 0] = shift(second_weight, z=3)
    weights[1, 1] = shift(weights[0, 1], z=1)
    weights[3, 1] = shift(weights[0, 1], z=3)
    weights[2, 0] = shift(weights[1, 0], z=1)
    weights[2, 1] = shift(weights[3, 1], z=3)
    weights = [weights[chunk] for chunk in CHUNKS]

    blocks = first_product(idx, routing, patches, norm_gain, norm_bias, first_weight, first_bias)
    head = {0: blocks[0]}
    tail = {0: jnp.concatenate([shift_dp(blocks[k], k) for k in range(1, BLOCKS)], axis=0)}
    for j in (1, 3, 2):
        head[j] = shift(head[0], y=j)
        tail[j] = shift(tail[0], y=j)

    def parts(pair):
        return [part[j] for j in pair for part in (head, tail)]

    send_a, rows_a = send_product(idx, parts((1, 3)), weights)
    send_b, rows_b = send_product(idx, parts((2, 0)), weights)
    stay_a, cross_a = keep_product(idx, rows_a, shift(send_a, c=1), weights, False)
    stay_2, stay_0, cross_2, cross_0 = keep_product(idx, rows_b, shift(send_b, c=1), weights, True)
    came_a = shift(cross_a, xh=1)
    came_2 = shift(cross_2, y=2, xh=1)
    came_0 = shift(cross_0, xh=1)
    stay_2 = shift(stay_2, y=2)
    sums_a = [
        (stay_a[at].astype(F32) + came_a[at].astype(F32)).astype(BF) for at in (slice(0, ROWS), slice(ROWS, 2 * ROWS))
    ]
    from_1 = shift(sums_a[0], y=3)
    from_3 = shift(sums_a[1], y=1)

    emb, text_sums = text_half(text_embeds)
    normed = norm_half(emb, over_tensor(text_sums), final_gain, 1)
    pieces = [stay_0, came_0, from_1, stay_2, came_2, from_3]
    emb, sums = splice(idx, routing, grids, pieces, second_bias, text_embeds, emb)
    normed = norm_half(emb, over_tensor(sums), final_gain, 0, normed)
    return (emb, normed)


def solution(mesh):
    mesh = Mesh(mesh.devices.reshape([SIZES[a] for a in AXES]), AXES)
    dp, tensor = ("z", "y", "xl"), ("xh", "c")
    placed = (
        P(dp, None),
        P(),
        P(),
        P(None, tensor),
        P(tensor),
        P(tensor, dp),
        P(tensor),
        P(dp, tensor),
        P(tensor),
        P(),
        P(),
    )
    return jax.shard_map(
        per_device,
        mesh=mesh,
        in_specs=placed,
        out_specs=(P(dp, tensor), P(dp, tensor)),
        check_vma=False,
    )
```
